32 devices in a mesh: wide: 8 (over z, x), narrow: 4 (over y, core).
Axes of the slice: x: 2, y: 2, z: 4, core: 2. Of those that a mesh axis runs over, the one named last changes fastest.
Arguments:
- payload: bfloat16 [131072, 128], P(('wide', 'narrow')), may hold values from -6 to 6
- first_key: int32 [131072], P(('wide', 'narrow')), may hold values from 0 to 1073741823
- second_key: int32 [131072], P(('wide', 'narrow')), may hold values from 0 to 1073741823
- live: int32 [131072], P(('wide', 'narrow')), may hold values from 0 to 1
- first_bucket: int32 [131072], P(('wide', 'narrow')), may hold values from 0 to 7, as said below
- second_bucket: int32 [131072], P(('wide', 'narrow')), may hold values from 0 to 3
Outputs:
- group_mean: bfloat16 [131072, 128], P(('wide', 'narrow'))
- duplicate_count: int32 [], replicated
The draws below stay inside these ranges and needn't reach their ends.
Inputs may be any that keep to these rules, and one draw needn't show every extreme that they name: Each device's rows name each pair (first_bucket, second_bucket) exactly 128 times; in every draw there is one bucket pair all of whose rows survive; other rows survive or not as `live` says.
All inputs are finite; a program needn't handle non-finite values.
Results may differ from the reference program's by a relative error of at most 0.001.
Values may be sent and summed in bfloat16 or wider, within the bound.
A program may use at most 64 MiB of HBM per device.

```python
import jax
import jax.numpy as jnp

COLS = 128
ROWS_DEV = 4096
GROUPS = 1024
ROWS = 131072
N_NARROW = 4
DEVICES = 32


def layout_draw(key):
    base = jax.random.fold_in(key, 11)
    keys = jax.random.split(base, 8)
    sources = jax.random.split(keys[0], DEVICES)
    per_slot = ROWS_DEV // DEVICES
    owner = jax.vmap(lambda source_key: jax.random.permutation(source_key, ROWS_DEV) // per_slot)(sources).reshape(-1).astype(jnp.int32)
    group = jax.random.randint(keys[1], (ROWS,), 0, GROUPS)
    half_count = DEVICES * (GROUPS // 2)
    high_part = jax.random.permutation(keys[2], half_count).astype(jnp.int32)
    low_part = jax.random.randint(keys[3], (half_count,), 0, 4096)
    table_one = high_part * 4096 + low_part
    owner_base = jax.random.randint(keys[4], (DEVICES,), 0, 67108864)
    raw_first = table_one[owner * (GROUPS // 2) + group // 2]
    lowest = jnp.min(raw_first)
    highest = jnp.max(raw_first)
    first = jnp.where(raw_first == highest, 1073741823, raw_first - lowest).astype(jnp.int32)
    second = owner_base[owner] * 16 + group % 16
    keep_rate = jax.random.randint(keys[5], (DEVICES,), 150, 1025)
    hottest = jax.random.randint(keys[6], (), 0, DEVICES)
    keep_rate = jnp.where(jnp.arange(DEVICES) == hottest, 1024, keep_rate)
    alive = (jax.random.randint(keys[7], (ROWS,), 0, 1024) < keep_rate[owner]).astype(jnp.int32)
    return (owner, first, second, alive)


def draw_first_key(key, part):
    return layout_draw(key)[1].astype(jnp.int32)


def draw_second_key(key, part):
    return layout_draw(key)[2].astype(jnp.int32)


def draw_live(key, part):
    return layout_draw(key)[3].astype(jnp.int32)


def draw_first_bucket(key, part):
    return (layout_draw(key)[0] // N_NARROW).astype(jnp.int32)


def draw_second_bucket(key, part):
    return (layout_draw(key)[0] % N_NARROW).astype(jnp.int32)


def steps_of(rng, dims, shards, smallest, largest):
    factor_of, own = 1.0, jax.random.fold_in(rng, 6)
    for axis_at, shards_of in shards:
        steps = jnp.exp(jax.random.uniform(jax.random.fold_in(own, axis_at), (shards_of,), jnp.float32, smallest / len(shards), largest / len(shards)))
        factor_of = factor_of * jnp.repeat(steps, dims[axis_at] // shards_of).reshape([-1 if axis == axis_at else 1 for axis in range(len(dims))])
    return factor_of


def gaussian(own_key, dims, scale, limit, cuts=(), kind=jnp.bfloat16):
    values = scale * jax.random.normal(own_key, dims, jnp.float32)
    if cuts:
        values = values * steps_of(own_key, dims, cuts, -0.22, 0.18)
    return jnp.clip(values, -limit, limit).astype(kind)


def setup_inputs(seed: int = 0) -> dict:
    key_list = jax.random.split(jax.random.key(seed), 7)
    return {
        "payload": gaussian(key_list[0], (ROWS, COLS), 1.0, 6.0, ((0, 32),)),
        "first_key": draw_first_key(jax.random.fold_in(key_list[6], 71), 0),
        "second_key": draw_second_key(jax.random.fold_in(key_list[6], 71), 0),
        "live": draw_live(jax.random.fold_in(key_list[6], 71), 0),
        "first_bucket": draw_first_bucket(jax.random.fold_in(key_list[6], 71), 0),
        "second_bucket": draw_second_bucket(jax.random.fold_in(key_list[6], 71), 0),
    }


def reference(payload, first_key, second_key, live, first_bucket, second_bucket):
    row_total = payload.shape[0]
    position = jnp.arange(row_total, dtype=jnp.int32)
    dead = (1 - live).astype(jnp.int32)
    sort_order = jnp.lexsort((position, second_key, first_key, second_bucket, first_bucket, dead))
    fields = jnp.stack([dead, first_bucket, second_bucket, first_key, second_key], 0)[:, sort_order]
    change = jnp.any(fields[:, 1:] != fields[:, :-1], axis=0)
    starts = jnp.concatenate([jnp.ones((1,), jnp.bool_), change])
    segment = (jnp.cumsum(starts.astype(jnp.int32)) - 1).astype(jnp.int32)
    live_sorted = live[sort_order].astype(jnp.float32)
    values = payload[sort_order].astype(jnp.float32) * live_sorted[:, None]
    sums = jax.ops.segment_sum(values, segment, num_segments=row_total)
    counts = jax.ops.segment_sum(live_sorted, segment, num_segments=row_total)
    mean_sorted = sums[segment] / jnp.maximum(counts[segment], 1.0)[:, None]
    group_mean = jnp.zeros_like(mean_sorted).at[sort_order].set(mean_sorted).astype(jnp.bfloat16)
    duplicate_count = jnp.sum(live_sorted * (1.0 - starts.astype(jnp.float32))).astype(jnp.int32)
    return group_mean, duplicate_count
```

```python
import functools

import jax
import jax.numpy as jnp
from jax import lax
from jax.experimental import pallas as pl
from jax.experimental.pallas import tpu as pltpu
from jax.sharding import PartitionSpec as P

MESH = pl.DeviceIdType.MESH
VMEM = pltpu.VMEM
SMEM = pltpu.SMEM


def place(flat, narrow_count):
    return {"wide": flat // narrow_count, "narrow": flat % narrow_count}


def my_flat(narrow_count):
    return lax.axis_index("wide") * narrow_count + lax.axis_index("narrow")


def greet_all(me, devices, narrow_count):
    barrier = pltpu.get_barrier_semaphore()

    def greet(step, carry):
        peer = (me + step) % devices
        pl.semaphore_signal(
            barrier, inc=1, device_id=place(peer, narrow_count), device_id_type=MESH
        )
        return carry

    lax.fori_loop(1, devices, greet, 0)
    pl.semaphore_wait(barrier, devices - 1)


def wait_bytes(ref, sem):
    pltpu.make_async_copy(ref, ref, sem).wait()


def send_block(src, dst, send_sem, recv_sem, peer, narrow_count):
    pltpu.make_async_remote_copy(
        src_ref=src,
        dst_ref=dst,
        send_sem=send_sem,
        recv_sem=recv_sem,
        device_id=place(peer, narrow_count),
        device_id_type=MESH,
    ).start()


def tags_kernel(devices, narrow_count, tags_ref, got_ref, send_sem, recv_sem):
    me = my_flat(narrow_count)
    greet_all(me, devices, narrow_count)
    pltpu.make_async_copy(tags_ref.at[me], got_ref.at[me], recv_sem).start()

    def send(step, carry):
        peer = (me + step) % devices
        send_block(tags_ref.at[peer], got_ref.at[me], send_sem, recv_sem, peer, narrow_count)
        return carry

    lax.fori_loop(1, devices, send, 0)
    wait_bytes(got_ref, recv_sem)
    wait_bytes(tags_ref.at[pl.ds(0, devices - 1)], send_sem)


def gather_kernel(unroll, order_ref, rows_ref, out_ref, wide_in, wide_out):
    count = rows_ref.shape[0]
    wide_in[...] = rows_ref[...].astype(jnp.float32)

    def move(step, carry):
        base = pl.multiple_of(step * unroll, unroll)
        for u in range(unroll):
            source = order_ref[base + u]
            wide_out[pl.ds(base + u, 1), :] = wide_in[pl.ds(source, 1), :]
        return carry

    lax.fori_loop(0, count // unroll, move, 0)
    out_ref[...] = wide_out[...].astype(out_ref.dtype)


def scatter_kernel(unroll, order_ref, rows_ref, out_ref, wide_in, wide_out):
    count = rows_ref.shape[0]
    wide_in[...] = rows_ref[...].astype(jnp.float32)

    def move(step, carry):
        base = pl.multiple_of(step * unroll, unroll)
        for u in range(unroll):
            target = order_ref[base + u]
            wide_out[pl.ds(target, 1), :] = wide_in[pl.ds(base + u, 1), :]
        return carry

    lax.fori_loop(0, count // unroll, move, 0)
    out_ref[...] = wide_out[...].astype(out_ref.dtype)


def permute_rows(kernel, order, rows):
    count, cols = rows.shape
    return pl.pallas_call(
        functools.partial(kernel, 16),
        out_shape=jax.ShapeDtypeStruct(rows.shape, rows.dtype),
        in_specs=[pl.BlockSpec(memory_space=SMEM), pl.BlockSpec(memory_space=VMEM)],
        out_specs=pl.BlockSpec(memory_space=VMEM),
        scratch_shapes=[VMEM((count, cols), jnp.float32), VMEM((count, cols), jnp.float32)],
    )(order, rows)


def exchange_kernel(
    devices, narrow_count, chunks, tile,
    rows_ref, key_one_ref, key_two_ref,
    back_ref, dup_ref,
    got, totals, means, col_one, col_two, lane_one, wide_rows, dup_mine, dup_all,
    send_sem, recv_sems, back_send, back_recv, dup_send, dup_recv,
):
    _, slot_rows, cols = rows_ref.shape
    count = devices * slot_rows
    chunk_slots = devices // chunks
    chunk_rows = chunk_slots * slot_rows
    lanes = key_one_ref.shape[1]
    me = my_flat(narrow_count)
    my_chunk = me // chunk_slots
    greet_all(me, devices, narrow_count)

    pltpu.make_async_copy(rows_ref.at[me], got.at[me], recv_sems.at[0]).start()
    for c in range(chunks):
        first = ((my_chunk + c) % chunks) * chunk_slots

        def send(step, carry, first=first, c=c):
            peer = first + (me + step) % chunk_slots
            send_block(
                rows_ref.at[peer], got.at[me], send_sem, recv_sems.at[c], peer, narrow_count
            )
            return carry

        lax.fori_loop(1 if c == 0 else 0, chunk_slots, send, 0)

    one = key_one_ref[...]
    lane_one[...] = jnp.where(one < 0, -2, one)
    flipped_one = one.T
    flipped_two = key_two_ref[...].T
    for r in range(count // lanes):
        at = pl.ds(r * lanes, lanes)
        col_one[at, :] = jnp.broadcast_to(flipped_one[:, r : r + 1], (lanes, lanes))
        col_two[at, :] = jnp.broadcast_to(flipped_two[:, r : r + 1], (lanes, lanes))
    wide_rows[:, cols:] = jnp.ones((chunk_rows, cols), wide_rows.dtype)
    dup_mine[...] = jnp.zeros_like(dup_mine)

    tiles = count // tile
    tile_slots = tile // slot_rows
    my_tile = me // tile_slots

    def send_tile(index):
        for u in range(tile_slots):
            peer = index * tile_slots + u

            @pl.when(peer == me)
            def _():
                pltpu.make_async_copy(means.at[peer], back_ref.at[me], back_recv).start()

            @pl.when(peer != me)
            def _():
                send_block(
                    means.at[peer], back_ref.at[me], back_send, back_recv, peer, narrow_count
                )

    for c in range(chunks):
        first = ((my_chunk - c + chunks) % chunks) * chunk_slots
        wait_bytes(got.at[pl.ds(first, chunk_slots)], recv_sems.at[c])
        wide_rows[:, :cols] = got[pl.ds(first, chunk_slots)].reshape(chunk_rows, cols)
        lane_base = first * slot_rows // lanes

        def body(step, carry, c=c, lane_base=lane_base):
            index = (my_tile + step) % tiles
            at = pl.ds(pl.multiple_of(index * tile, tile), tile)
            left_one = col_one[at, :]
            left_two = col_two[at, :]
            parts = []
            for b in range(chunk_rows // lanes):
                row_at = pl.ds(lane_base + b, 1)
                same = (left_one == lane_one[row_at, :]) & (left_two == key_two_ref[row_at, :])
                parts.append(jnp.where(same, 1.0, 0.0).astype(jnp.bfloat16))
            mask = jnp.concatenate(parts, axis=1)
            part = jnp.dot(mask, wide_rows[...], preferred_element_type=jnp.float32)
            if c > 0:
                part = part + totals[at, :]
            if c < chunks - 1:
                totals[at, :] = part
            else:
                sums = part[:, :cols]
                counts = part[:, cols:]
                floor = jnp.maximum(counts, 1.0)
                mean = (sums / floor).astype(means.dtype)
                means[pl.ds(index * tile_slots, tile_slots)] = mean.reshape(
                    tile_slots, slot_rows, cols
                )
                held = jnp.where(counts > 0.0, 1.0, 0.0)
                dup_mine[0] += jnp.sum(held.reshape(tile // 8, 8, cols), axis=0)
                dup_mine[1] += jnp.sum((held / floor).reshape(tile // 8, 8, cols), axis=0)

                @pl.when(step > 0)
                def _():
                    send_tile((my_tile + step + tiles - 1) % tiles)
            return carry

        lax.fori_loop(0, tiles, body, 0)

    live_rows = jnp.sum(dup_mine[0], axis=0, keepdims=True)
    groups = jnp.floor(jnp.sum(dup_mine[1], axis=0, keepdims=True) + 0.5)
    dup_mine[0] = jnp.broadcast_to(live_rows - groups, (8, cols))
    send_tile((my_tile + tiles - 1) % tiles)
    pltpu.make_async_copy(dup_mine.at[0], dup_all.at[me], dup_recv).start()

    def send_dup(step, carry):
        peer = (me + step) % devices
        send_block(dup_mine.at[0], dup_all.at[me], dup_send, dup_recv, peer, narrow_count)
        return carry

    lax.fori_loop(1, devices, send_dup, 0)
    wait_bytes(dup_all, dup_recv)
    dup_ref[...] = jnp.sum(dup_all[...], axis=0).astype(jnp.int32)
    wait_bytes(back_ref, back_recv)
    wait_bytes(rows_ref.at[pl.ds(0, devices - 1)], send_sem)
    wait_bytes(means.at[pl.ds(0, devices - 1)], back_send)
    wait_bytes(dup_all.at[pl.ds(0, devices - 1)], dup_send)


def on_device(payload, first_key, second_key, live, first_bucket, second_bucket):
    wide_count = lax.axis_size("wide")
    narrow_count = lax.axis_size("narrow")
    devices = wide_count * narrow_count
    row_count, cols = payload.shape
    slot_rows = row_count // devices
    owner = first_bucket * narrow_count + second_bucket
    packed = owner * row_count + lax.iota(jnp.int32, row_count)
    packed, key_one, key_two = lax.sort(
        (packed, jnp.where(live > 0, first_key, -1), second_key), num_keys=1, is_stable=False
    )
    order = packed % row_count
    tags = jnp.stack(
        [key_one.reshape(devices, slot_rows), key_two.reshape(devices, slot_rows)], axis=1
    ).reshape(devices, 1, 2 * slot_rows)
    got_tags = pl.pallas_call(
        functools.partial(tags_kernel, devices, narrow_count),
        out_shape=jax.ShapeDtypeStruct(tags.shape, tags.dtype),
        in_specs=[pl.BlockSpec(memory_space=VMEM)],
        out_specs=pl.BlockSpec(memory_space=VMEM),
        scratch_shapes=[pltpu.SemaphoreType.DMA, pltpu.SemaphoreType.DMA],
        compiler_params=pltpu.CompilerParams(collective_id=0, has_side_effects=True),
    )(tags)
    lanes = 128
    keys_one = got_tags[:, 0, :slot_rows].reshape(row_count // lanes, lanes)
    keys_two = got_tags[:, 0, slot_rows:].reshape(row_count // lanes, lanes)
    sent = permute_rows(gather_kernel, order, payload).reshape(devices, slot_rows, cols)

    chunks = 4 if devices % 4 == 0 else 1
    tile = max(256, slot_rows)
    tile = min(tile, row_count)
    block = (devices, slot_rows, cols)
    back, dups = pl.pallas_call(
        functools.partial(exchange_kernel, devices, narrow_count, chunks, tile),
        out_shape=(
            jax.ShapeDtypeStruct(block, payload.dtype),
            jax.ShapeDtypeStruct((8, cols), jnp.int32),
        ),
        in_specs=[pl.BlockSpec(memory_space=VMEM)] * 3,
        out_specs=(pl.BlockSpec(memory_space=VMEM), pl.BlockSpec(memory_space=VMEM)),
        scratch_shapes=[
            VMEM(block, payload.dtype),
            VMEM((row_count, 2 * cols), jnp.float32),
            VMEM(block, payload.dtype),
            VMEM((row_count, lanes), jnp.int32),
            VMEM((row_count, lanes), jnp.int32),
            VMEM((row_count // lanes, lanes), jnp.int32),
            VMEM((row_count // chunks, 2 * cols), payload.dtype),
            VMEM((2, 8, cols), jnp.float32),
            VMEM((devices, 8, cols), jnp.float32),
            pltpu.SemaphoreType.DMA,
            pltpu.SemaphoreType.DMA((chunks,)),
            pltpu.SemaphoreType.DMA,
            pltpu.SemaphoreType.DMA,
            pltpu.SemaphoreType.DMA,
            pltpu.SemaphoreType.DMA,
        ],
        compiler_params=pltpu.CompilerParams(
            collective_id=1, has_side_effects=True, vmem_limit_bytes=48 * 1024 * 1024
        ),
    )(sent, keys_one, keys_two)
    group_mean = permute_rows(scatter_kernel, order, back.reshape(row_count, cols))
    return (group_mean, dups[0, 0])


def solution(mesh):
    placed = (
        P(("wide", "narrow"), None),
        P(("wide", "narrow")),
        P(("wide", "narrow")),
        P(("wide", "narrow")),
        P(("wide", "narrow")),
        P(("wide", "narrow")),
    )
    return jax.shard_map(
        on_device,
        mesh=mesh,
        in_specs=placed,
        out_specs=(P(("wide", "narrow"), None), P()),
        check_vma=False,
    )
```

```python
import functools

import jax
import jax.numpy as jnp
from jax import lax
from jax.experimental import pallas as pl
from jax.experimental.pallas import tpu as pltpu
from jax.sharding import PartitionSpec as P

MESH = pl.DeviceIdType.MESH
VMEM = pltpu.VMEM
SMEM = pltpu.SMEM


def place(flat, narrow_count):
    return {"wide": flat // narrow_count, "narrow": flat % narrow_count}


def my_flat(narrow_count):
    return lax.axis_index("wide") * narrow_count + lax.axis_index("narrow")


def greet_all(me, devices, narrow_count):
    barrier = pltpu.get_barrier_semaphore()

    def greet(step, carry):
        peer = (me + step) % devices
        pl.semaphore_signal(
            barrier, inc=1, device_id=place(peer, narrow_count), device_id_type=MESH
        )
        return carry

    lax.fori_loop(1, devices, greet, 0)
    return barrier


def wait_bytes(ref, sem):
    pltpu.make_async_copy(ref, ref, sem).wait()


def send_block(src, dst, send_sem, recv_sem, peer, narrow_count):
    pltpu.make_async_remote_copy(
        src_ref=src,
        dst_ref=dst,
        send_sem=send_sem,
        recv_sem=recv_sem,
        device_id=place(peer, narrow_count),
        device_id_type=MESH,
    ).start()


def scatter_kernel(unroll, order_ref, rows_ref, out_ref, wide_in, wide_out):
    count = rows_ref.shape[0]
    wide_in[...] = rows_ref[...].astype(jnp.float32)

    def move(step, carry):
        base = pl.multiple_of(step * unroll, unroll)
        for u in range(unroll):
            target = order_ref[base + u]
            wide_out[pl.ds(target, 1), :] = wide_in[pl.ds(base + u, 1), :]
        return carry

    lax.fori_loop(0, count // unroll, move, 0)
    out_ref[...] = wide_out[...].astype(out_ref.dtype)


def scatter_rows(order, rows):
    count, cols = rows.shape
    return pl.pallas_call(
        functools.partial(scatter_kernel, 16),
        out_shape=jax.ShapeDtypeStruct(rows.shape, rows.dtype),
        in_specs=[pl.BlockSpec(memory_space=SMEM), pl.BlockSpec(memory_space=VMEM)],
        out_specs=pl.BlockSpec(memory_space=VMEM),
        scratch_shapes=[VMEM((count, cols), jnp.float32), VMEM((count, cols), jnp.float32)],
    )(order, rows)


def exchange_kernel(
    devices, narrow_count, chunks, tile,
    order_ref, payload_ref, sent_one, sent_two,
    back_ref, dup_ref,
    rows_ref, wide_in, wide_slot, got_one, got_two,
    got, totals, means, col_one, col_two, lane_one, lane_two, wide_rows, dup_mine, dup_all,
    tag_send, tag_recv,
    send_sem, recv_sems, back_send, back_recv, dup_send, dup_recv,
):
    _, slot_rows, cols = rows_ref.shape
    count = devices * slot_rows
    chunk_slots = devices // chunks
    chunk_rows = chunk_slots * slot_rows
    lanes = lane_one.shape[1]
    me = my_flat(narrow_count)
    my_chunk = me // chunk_slots
    barrier = greet_all(me, devices, narrow_count)
    wide_in[...] = payload_ref[...].astype(jnp.float32)
    pl.semaphore_wait(barrier, devices - 1)

    pltpu.make_async_copy(sent_one.at[me], got_one.at[me], tag_recv.at[0]).start()
    pltpu.make_async_copy(sent_two.at[me], got_two.at[me], tag_recv.at[1]).start()

    def send_tags(step, carry):
        peer = (me + step) % devices
        send_block(
            sent_one.at[peer], got_one.at[me], tag_send.at[0], tag_recv.at[0], peer, narrow_count
        )
        send_block(
            sent_two.at[peer], got_two.at[me], tag_send.at[1], tag_recv.at[1], peer, narrow_count
        )
        return carry

    lax.fori_loop(1, devices, send_tags, 0)

    def peer_of(step):
        chunk = step // chunk_slots
        first = ((my_chunk + chunk) % chunks) * chunk_slots
        return chunk, first + (me + step) % chunk_slots

    def send_slot(step):
        chunk, peer = peer_of(step)
        send_block(
            rows_ref.at[peer], got.at[me], send_sem, recv_sems.at[chunk], peer, narrow_count
        )

    unroll = min(16, slot_rows)

    def fill(step, carry):
        _, peer = peer_of(step)

        def move(inner, carry):
            base = pl.multiple_of(inner * unroll, unroll)
            for u in range(unroll):
                source = order_ref[peer * slot_rows + base + u]
                wide_slot[pl.ds(base + u, 1), :] = wide_in[pl.ds(source, 1), :]
            return carry

        lax.fori_loop(0, slot_rows // unroll, move, 0)
        rows_ref[peer] = wide_slot[...].astype(rows_ref.dtype)

        @pl.when(step > 1)
        def _():
            send_slot(step - 1)

        return carry

    lax.fori_loop(0, devices, fill, 0)
    pltpu.make_async_copy(rows_ref.at[me], got.at[me], recv_sems.at[0]).start()

    wait_bytes(got_one, tag_recv.at[0])
    send_slot(devices - 1)
    wait_bytes(got_two, tag_recv.at[1])
    if slot_rows >= lanes:
        per_slot = slot_rows // lanes
        for r in range(count // lanes):
            piece = pl.ds(r % per_slot * lanes, lanes)
            lane_one[r : r + 1, :] = got_one[r // per_slot, :, piece]
            lane_two[r : r + 1, :] = got_two[r // per_slot, :, piece]
    else:
        group = lanes // slot_rows
        for r in range(count // lanes):
            pieces = range(r * group, (r + 1) * group)
            lane_one[r : r + 1, :] = jnp.concatenate([got_one[p] for p in pieces], axis=1)
            lane_two[r : r + 1, :] = jnp.concatenate([got_two[p] for p in pieces], axis=1)
    one = lane_one[...]
    flipped_one = one.T
    flipped_two = lane_two[...].T
    lane_one[...] = jnp.where(one < 0, -2, one)
    for r in range(count // lanes):
        at = pl.ds(r * lanes, lanes)
        col_one[at, :] = jnp.broadcast_to(flipped_one[:, r : r + 1], (lanes, lanes))
        col_two[at, :] = jnp.broadcast_to(flipped_two[:, r : r + 1], (lanes, lanes))
    wide_rows[:, cols:] = jnp.ones((chunk_rows, cols), wide_rows.dtype)
    dup_mine[...] = jnp.zeros_like(dup_mine)

    tiles = count // tile
    tile_slots = tile // slot_rows
    my_tile = me // tile_slots

    def send_tile(index):
        for u in range(tile_slots):
            peer = index * tile_slots + u

            @pl.when(peer == me)
            def _():
                pltpu.make_async_copy(means.at[peer], back_ref.at[me], back_recv).start()

            @pl.when(peer != me)
            def _():
                send_block(
                    means.at[peer], back_ref.at[me], back_send, back_recv, peer, narrow_count
                )

    for c in range(chunks):
        first = ((my_chunk - c + chunks) % chunks) * chunk_slots
        wait_bytes(got.at[pl.ds(first, chunk_slots)], recv_sems.at[c])
        wide_rows[:, :cols] = got[pl.ds(first, chunk_slots)].reshape(chunk_rows, cols)
        lane_base = first * slot_rows // lanes

        def body(step, carry, c=c, lane_base=lane_base):
            index = (my_tile + step) % tiles
            at = pl.ds(pl.multiple_of(index * tile, tile), tile)
            left_one = col_one[at, :]
            left_two = col_two[at, :]
            parts = []
            for b in range(chunk_rows // lanes):
                row_at = pl.ds(lane_base + b, 1)
                same = (left_one == lane_one[row_at, :]) & (left_two == lane_two[row_at, :])
                parts.append(jnp.where(same, 1.0, 0.0).astype(jnp.bfloat16))
            mask = jnp.concatenate(parts, axis=1)
            part = jnp.dot(mask, wide_rows[...], preferred_element_type=jnp.float32)
            if c > 0:
                part = part + totals[at, :]
            if c < chunks - 1:
                totals[at, :] = part
            else:
                sums = part[:, :cols]
                counts = part[:, cols:]
                floor = jnp.maximum(counts, 1.0)
                mean = (sums / floor).astype(means.dtype)
                means[pl.ds(index * tile_slots, tile_slots)] = mean.reshape(
                    tile_slots, slot_rows, cols
                )
                held = jnp.where(counts > 0.0, 1.0, 0.0)
                dup_mine[0] += jnp.sum(held.reshape(tile // 8, 8, cols), axis=0)
                dup_mine[1] += jnp.sum((held / floor).reshape(tile // 8, 8, cols), axis=0)

                @pl.when(step > 0)
                def _():
                    send_tile((my_tile + step + tiles - 1) % tiles)
            return carry

        lax.fori_loop(0, tiles, body, 0)

    live_rows = jnp.sum(dup_mine[0], axis=0, keepdims=True)
    groups = jnp.floor(jnp.sum(dup_mine[1], axis=0, keepdims=True) + 0.5)
    dup_mine[0] = jnp.broadcast_to(live_rows - groups, (8, cols))
    send_tile((my_tile + tiles - 1) % tiles)
    pltpu.make_async_copy(dup_mine.at[0], dup_all.at[me], dup_recv).start()

    def send_dup(step, carry):
        peer = (me + step) % devices
        send_block(dup_mine.at[0], dup_all.at[me], dup_send, dup_recv, peer, narrow_count)
        return carry

    lax.fori_loop(1, devices, send_dup, 0)
    wait_bytes(dup_all, dup_recv)
    dup_ref[...] = jnp.sum(dup_all[...], axis=0).astype(jnp.int32)
    wait_bytes(back_ref, back_recv)
    wait_bytes(sent_one.at[pl.ds(0, devices - 1)], tag_send.at[0])
    wait_bytes(sent_two.at[pl.ds(0, devices - 1)], tag_send.at[1])
    wait_bytes(rows_ref.at[pl.ds(0, devices - 1)], send_sem)
    wait_bytes(means.at[pl.ds(0, devices - 1)], back_send)
    wait_bytes(dup_all.at[pl.ds(0, devices - 1)], dup_send)


def on_device(payload, first_key, second_key, live, first_bucket, second_bucket):
    wide_count = lax.axis_size("wide")
    narrow_count = lax.axis_size("narrow")
    devices = wide_count * narrow_count
    row_count, cols = payload.shape
    slot_rows = row_count // devices
    owner = first_bucket * narrow_count + second_bucket
    packed = owner * row_count + lax.iota(jnp.int32, row_count)
    packed, key_one, key_two = lax.sort(
        (packed, jnp.where(live > 0, first_key, -1), second_key), num_keys=1, is_stable=False
    )
    order = packed % row_count
    lanes = 128
    tags = (devices, 1, slot_rows)
    chunks = 4 if devices % 4 == 0 else 1
    tile = max(256, slot_rows)
    tile = min(tile, row_count)
    block = (devices, slot_rows, cols)
    back, dups = pl.pallas_call(
        functools.partial(exchange_kernel, devices, narrow_count, chunks, tile),
        out_shape=(
            jax.ShapeDtypeStruct(block, payload.dtype),
            jax.ShapeDtypeStruct((8, cols), jnp.int32),
        ),
        in_specs=[pl.BlockSpec(memory_space=SMEM)] + [pl.BlockSpec(memory_space=VMEM)] * 3,
        out_specs=(pl.BlockSpec(memory_space=VMEM), pl.BlockSpec(memory_space=VMEM)),
        scratch_shapes=[
            VMEM(block, payload.dtype),
            VMEM((row_count, cols), jnp.float32),
            VMEM((slot_rows, cols), jnp.float32),
            VMEM(tags, jnp.int32),
            VMEM(tags, jnp.int32),
            VMEM(block, payload.dtype),
            VMEM((row_count, 2 * cols), jnp.float32),
            VMEM(block, payload.dtype),
            VMEM((row_count, lanes), jnp.int32),
            VMEM((row_count, lanes), jnp.int32),
            VMEM((row_count // lanes, lanes), jnp.int32),
            VMEM((row_count // lanes, lanes), jnp.int32),
            VMEM((row_count // chunks, 2 * cols), payload.dtype),
            VMEM((2, 8, cols), jnp.float32),
            VMEM((devices, 8, cols), jnp.float32),
            pltpu.SemaphoreType.DMA((2,)),
            pltpu.SemaphoreType.DMA((2,)),
            pltpu.SemaphoreType.DMA,
            pltpu.SemaphoreType.DMA((chunks,)),
            pltpu.SemaphoreType.DMA,
            pltpu.SemaphoreType.DMA,
            pltpu.SemaphoreType.DMA,
            pltpu.SemaphoreType.DMA,
        ],
        compiler_params=pltpu.CompilerParams(
            collective_id=0, has_side_effects=True, vmem_limit_bytes=48 * 1024 * 1024
        ),
    )(order, payload, key_one.reshape(tags), key_two.reshape(tags))
    group_mean = scatter_rows(order, back.reshape(row_count, cols))
    return (group_mean, dups[0, 0])


def solution(mesh):
    placed = (
        P(("wide", "narrow"), None),
        P(("wide", "narrow")),
        P(("wide", "narrow")),
        P(("wide", "narrow")),
        P(("wide", "narrow")),
        P(("wide", "narrow")),
    )
    return jax.shard_map(
        on_device,
        mesh=mesh,
        in_specs=placed,
        out_specs=(P(("wide", "narrow"), None), P()),
        check_vma=False,
    )
```

```python
import functools

import jax
import jax.numpy as jnp
from jax import lax
from jax.experimental import pallas as pl
from jax.experimental.pallas import tpu as pltpu
from jax.sharding import PartitionSpec as P

MESH = pl.DeviceIdType.MESH
VMEM = pltpu.VMEM
SMEM = pltpu.SMEM


def place(flat, narrow_count):
    return {"wide": flat // narrow_count, "narrow": flat % narrow_count}


def my_flat(narrow_count):
    return lax.axis_index("wide") * narrow_count + lax.axis_index("narrow")


def greet_all(me, devices, narrow_count):
    barrier = pltpu.get_barrier_semaphore()

    def greet(step, carry):
        peer = (me + step) % devices
        pl.semaphore_signal(
            barrier, inc=1, device_id=place(peer, narrow_count), device_id_type=MESH
        )
        return carry

    lax.fori_loop(1, devices, greet, 0)
    return barrier


def wait_bytes(ref, sem):
    pltpu.make_async_copy(ref, ref, sem).wait()


def send_block(src, dst, send_sem, recv_sem, peer, narrow_count):
    pltpu.make_async_remote_copy(
        src_ref=src,
        dst_ref=dst,
        send_sem=send_sem,
        recv_sem=recv_sem,
        device_id=place(peer, narrow_count),
        device_id_type=MESH,
    ).start()


def scatter_kernel(unroll, parts, order_ref, dups_ref, rows_any, out_ref, dup_ref,
                   rows_in, wide_in, wide_out, sems):
    count = rows_in.shape[0]
    part = count // parts
    copies = [
        pltpu.make_async_copy(
            rows_any.at[pl.ds(p * part, part)], rows_in.at[pl.ds(p * part, part)], sems.at[p]
        )
        for p in range(parts)
    ]
    for copy in copies:
        copy.start()
    dup_ref[0] = dups_ref[0, 0]

    def move(step, carry):
        base = pl.multiple_of(step * unroll, unroll)
        for u in range(unroll):
            target = order_ref[base + u]
            wide_out[pl.ds(target, 1), :] = wide_in[pl.ds(base + u, 1), :]
        return carry

    for p, copy in enumerate(copies):
        copy.wait()
        at = pl.ds(p * part, part)
        wide_in[at, :] = rows_in[at, :].astype(jnp.float32)
        lax.fori_loop(p * part // unroll, (p + 1) * part // unroll, move, 0)
    out_ref[...] = wide_out[...].astype(out_ref.dtype)


def scatter_rows(order, dups, rows):
    count, cols = rows.shape
    parts = 4
    return pl.pallas_call(
        functools.partial(scatter_kernel, 16, parts),
        out_shape=(
            jax.ShapeDtypeStruct(rows.shape, rows.dtype),
            jax.ShapeDtypeStruct((1,), jnp.int32),
        ),
        in_specs=[
            pl.BlockSpec(memory_space=SMEM),
            pl.BlockSpec(memory_space=VMEM),
            pl.BlockSpec(memory_space=pl.ANY),
        ],
        out_specs=(pl.BlockSpec(memory_space=VMEM), pl.BlockSpec(memory_space=SMEM)),
        scratch_shapes=[
            VMEM((count, cols), rows.dtype),
            VMEM((count, cols), jnp.float32),
            VMEM((count, cols), jnp.float32),
            pltpu.SemaphoreType.DMA((parts,)),
        ],
        compiler_params=pltpu.CompilerParams(vmem_limit_bytes=16 * 1024 * 1024),
    )(order, dups, rows)


def exchange_kernel(
    devices, narrow_count, chunks, tile,
    order_ref, payload_any, sent_one, sent_two,
    back_ref, dup_ref,
    rows_ref, wide_in, wide_slot, got_one, got_two,
    got, totals, means, col_one, col_two, lane_one, lane_two, wide_rows, dup_mine, dup_all,
    payload_ref, load_sem, tag_send, tag_recv,
    send_sem, recv_sems, back_send, back_recv, dup_send, dup_recv,
):
    _, slot_rows, cols = rows_ref.shape
    count = devices * slot_rows
    chunk_slots = devices // chunks
    chunk_rows = chunk_slots * slot_rows
    lanes = lane_one.shape[1]
    me = my_flat(narrow_count)
    my_chunk = me // chunk_slots
    load = pltpu.make_async_copy(payload_any, payload_ref, load_sem)
    load.start()
    barrier = greet_all(me, devices, narrow_count)
    load.wait()
    wide_in[...] = payload_ref[...].astype(jnp.float32)
    pl.semaphore_wait(barrier, devices - 1)

    pltpu.make_async_copy(sent_one.at[me], got_one.at[me], tag_recv.at[0]).start()
    pltpu.make_async_copy(sent_two.at[me], got_two.at[me], tag_recv.at[1]).start()

    def send_tags(step, carry):
        peer = (me + step) % devices
        send_block(
            sent_one.at[peer], got_one.at[me], tag_send.at[0], tag_recv.at[0], peer, narrow_count
        )
        send_block(
            sent_two.at[peer], got_two.at[me], tag_send.at[1], tag_recv.at[1], peer, narrow_count
        )
        return carry

    lax.fori_loop(1, devices, send_tags, 0)

    def peer_of(step):
        chunk = step // chunk_slots
        first = ((my_chunk + 1 + chunk) % chunks) * chunk_slots
        return chunk, first + (me + 1 + step) % chunk_slots

    def send_slot(step):
        chunk, peer = peer_of(step)
        send_block(
            rows_ref.at[peer], got.at[me], send_sem, recv_sems.at[chunk], peer, narrow_count
        )

    unroll = min(16, slot_rows)

    def fill(step, carry):
        _, peer = peer_of(step)

        def move(inner, carry):
            base = pl.multiple_of(inner * unroll, unroll)
            for u in range(unroll):
                source = order_ref[peer * slot_rows + base + u]
                wide_slot[pl.ds(base + u, 1), :] = wide_in[pl.ds(source, 1), :]
            return carry

        lax.fori_loop(0, slot_rows // unroll, move, 0)
        rows_ref[peer] = wide_slot[...].astype(rows_ref.dtype)

        @pl.when(step > 0)
        def _():
            send_slot(step - 1)

        return carry

    lax.fori_loop(0, devices, fill, 0)
    pltpu.make_async_copy(rows_ref.at[me], got.at[me], recv_sems.at[chunks - 1]).start()

    wait_bytes(got_one, tag_recv.at[0])
    wait_bytes(got_two, tag_recv.at[1])
    if slot_rows >= lanes:
        per_slot = slot_rows // lanes
        for r in range(count // lanes):
            piece = pl.ds(r % per_slot * lanes, lanes)
            lane_one[r : r + 1, :] = got_one[r // per_slot, :, piece]
            lane_two[r : r + 1, :] = got_two[r // per_slot, :, piece]
    else:
        group = lanes // slot_rows
        for r in range(count // lanes):
            pieces = range(r * group, (r + 1) * group)
            lane_one[r : r + 1, :] = jnp.concatenate([got_one[p] for p in pieces], axis=1)
            lane_two[r : r + 1, :] = jnp.concatenate([got_two[p] for p in pieces], axis=1)
    one = lane_one[...]
    flipped_one = one.T
    flipped_two = lane_two[...].T
    lane_one[...] = jnp.where(one < 0, -2, one)
    for r in range(count // lanes):
        at = pl.ds(r * lanes, lanes)
        col_one[at, :] = jnp.broadcast_to(flipped_one[:, r : r + 1], (lanes, lanes))
        col_two[at, :] = jnp.broadcast_to(flipped_two[:, r : r + 1], (lanes, lanes))
    wide_rows[:, cols:] = jnp.ones((chunk_rows, cols), wide_rows.dtype)
    dup_mine[...] = jnp.zeros_like(dup_mine)

    tiles = count // tile
    tile_slots = tile // slot_rows
    lead = me // tile_slots + max(1, tiles // chunks)

    def send_tile(index):
        for u in range(tile_slots):
            peer = index * tile_slots + u

            @pl.when(peer == me)
            def _():
                pltpu.make_async_copy(means.at[peer], back_ref.at[me], back_recv).start()

            @pl.when(peer != me)
            def _():
                send_block(
                    means.at[peer], back_ref.at[me], back_send, back_recv, peer, narrow_count
                )

    turns = list(range(chunks))
    if chunks > 2:
        turns = turns[: chunks - 2] + [chunks - 1, chunks - 2]
    for turn, c in enumerate(turns):
        first = ((my_chunk - 1 - c + 2 * chunks) % chunks) * chunk_slots
        wait_bytes(got.at[pl.ds(first, chunk_slots)], recv_sems.at[c])
        wide_rows[:, :cols] = got[pl.ds(first, chunk_slots)].reshape(chunk_rows, cols)
        lane_base = first * slot_rows // lanes

        def body(step, carry, turn=turn, lane_base=lane_base):
            index = (lead + step) % tiles
            at = pl.ds(pl.multiple_of(index * tile, tile), tile)
            left_one = col_one[at, :]
            left_two = col_two[at, :]
            parts = []
            for b in range(chunk_rows // lanes):
                row_at = pl.ds(lane_base + b, 1)
                same = (left_one == lane_one[row_at, :]) & (left_two == lane_two[row_at, :])
                parts.append(jnp.where(same, 1.0, 0.0).astype(jnp.bfloat16))
            mask = jnp.concatenate(parts, axis=1)
            part = jnp.dot(mask, wide_rows[...], preferred_element_type=jnp.float32)
            if turn > 0:
                part = part + totals[at, :]
            if turn < chunks - 1:
                totals[at, :] = part
            else:
                sums = part[:, :cols]
                counts = part[:, cols:]
                floor = jnp.maximum(counts, 1.0)
                mean = (sums / floor).astype(means.dtype)
                means[pl.ds(index * tile_slots, tile_slots)] = mean.reshape(
                    tile_slots, slot_rows, cols
                )
                held = jnp.where(counts > 0.0, 1.0, 0.0)
                dup_mine[0] += jnp.sum(held.reshape(tile // 8, 8, cols), axis=0)
                dup_mine[1] += jnp.sum((held / floor).reshape(tile // 8, 8, cols), axis=0)

                @pl.when(step > 0)
                def _():
                    send_tile((lead + step + tiles - 1) % tiles)
            return carry

        lax.fori_loop(0, tiles, body, 0)

    live_rows = jnp.sum(dup_mine[0], axis=0, keepdims=True)
    groups = jnp.floor(jnp.sum(dup_mine[1], axis=0, keepdims=True) + 0.5)
    dup_mine[0] = jnp.broadcast_to(live_rows - groups, (8, cols))
    send_tile((lead + tiles - 1) % tiles)
    pltpu.make_async_copy(dup_mine.at[0], dup_all.at[me], dup_recv).start()

    def send_dup(step, carry):
        peer = (me + step) % devices
        send_block(dup_mine.at[0], dup_all.at[me], dup_send, dup_recv, peer, narrow_count)
        return carry

    lax.fori_loop(1, devices, send_dup, 0)
    wait_bytes(dup_all, dup_recv)
    dup_ref[...] = jnp.sum(dup_all[...], axis=0).astype(jnp.int32)
    wait_bytes(back_ref, back_recv)
    wait_bytes(sent_one.at[pl.ds(0, devices - 1)], tag_send.at[0])
    wait_bytes(sent_two.at[pl.ds(0, devices - 1)], tag_send.at[1])
    wait_bytes(rows_ref.at[pl.ds(0, devices - 1)], send_sem)
    wait_bytes(means.at[pl.ds(0, devices - 1)], back_send)
    wait_bytes(dup_all.at[pl.ds(0, devices - 1)], dup_send)


def on_device(payload, first_key, second_key, live, first_bucket, second_bucket):
    wide_count = lax.axis_size("wide")
    narrow_count = lax.axis_size("narrow")
    devices = wide_count * narrow_count
    row_count, cols = payload.shape
    slot_rows = row_count // devices
    owner = first_bucket * narrow_count + second_bucket
    packed = owner * row_count + lax.iota(jnp.int32, row_count)
    packed, key_one, key_two = lax.sort(
        (packed, jnp.where(live > 0, first_key, -1), second_key), num_keys=1, is_stable=False
    )
    order = packed % row_count
    lanes = 128
    tags = (devices, 1, slot_rows)
    chunks = 4 if devices % 4 == 0 else 1
    tile = max(256, slot_rows)
    tile = min(tile, row_count)
    block = (devices, slot_rows, cols)
    back, dups = pl.pallas_call(
        functools.partial(exchange_kernel, devices, narrow_count, chunks, tile),
        out_shape=(
            jax.ShapeDtypeStruct(block, payload.dtype),
            jax.ShapeDtypeStruct((8, cols), jnp.int32),
        ),
        in_specs=[
            pl.BlockSpec(memory_space=SMEM),
            pl.BlockSpec(memory_space=pltpu.HBM),
            pl.BlockSpec(memory_space=VMEM),
            pl.BlockSpec(memory_space=VMEM),
        ],
        out_specs=(pl.BlockSpec(memory_space=VMEM), pl.BlockSpec(memory_space=VMEM)),
        scratch_shapes=[
            VMEM(block, payload.dtype),
            VMEM((row_count, cols), jnp.float32),
            VMEM((slot_rows, cols), jnp.float32),
            VMEM(tags, jnp.int32),
            VMEM(tags, jnp.int32),
            VMEM(block, payload.dtype),
            VMEM((row_count, 2 * cols), jnp.float32),
            VMEM(block, payload.dtype),
            VMEM((row_count, lanes), jnp.int32),
            VMEM((row_count, lanes), jnp.int32),
            VMEM((row_count // lanes, lanes), jnp.int32),
            VMEM((row_count // lanes, lanes), jnp.int32),
            VMEM((row_count // chunks, 2 * cols), payload.dtype),
            VMEM((2, 8, cols), jnp.float32),
            VMEM((devices, 8, cols), jnp.float32),
            VMEM((row_count, cols), payload.dtype),
            pltpu.SemaphoreType.DMA,
            pltpu.SemaphoreType.DMA((2,)),
            pltpu.SemaphoreType.DMA((2,)),
            pltpu.SemaphoreType.DMA,
            pltpu.SemaphoreType.DMA((chunks,)),
            pltpu.SemaphoreType.DMA,
            pltpu.SemaphoreType.DMA,
            pltpu.SemaphoreType.DMA,
            pltpu.SemaphoreType.DMA,
        ],
        compiler_params=pltpu.CompilerParams(
            collective_id=0, has_side_effects=True, vmem_limit_bytes=48 * 1024 * 1024
        ),
    )(order, payload, key_one.reshape(tags), key_two.reshape(tags))
    group_mean, total = scatter_rows(order, dups, back.reshape(row_count, cols))
    return (group_mean, total[0])


def solution(mesh):
    placed = (
        P(("wide", "narrow"), None),
        P(("wide", "narrow")),
        P(("wide", "narrow")),
        P(("wide", "narrow")),
        P(("wide", "narrow")),
        P(("wide", "narrow")),
    )
    return jax.shard_map(
        on_device,
        mesh=mesh,
        in_specs=placed,
        out_specs=(P(("wide", "narrow"), None), P()),
        check_vma=False,
    )
```

```python
import functools

import jax
import jax.numpy as jnp
from jax import lax
from jax.experimental import pallas as pl
from jax.experimental.pallas import tpu as pltpu
from jax.sharding import PartitionSpec as P

MESH = pl.DeviceIdType.MESH
VMEM = pltpu.VMEM
SMEM = pltpu.SMEM


def place(flat, narrow_count):
    return {"wide": flat // narrow_count, "narrow": flat % narrow_count}


def my_flat(narrow_count):
    return lax.axis_index("wide") * narrow_count + lax.axis_index("narrow")


def greet_all(me, devices, narrow_count):
    barrier = pltpu.get_barrier_semaphore()

    def greet(step, carry):
        peer = (me + step) % devices
        pl.semaphore_signal(
            barrier, inc=1, device_id=place(peer, narrow_count), device_id_type=MESH
        )
        return carry

    lax.fori_loop(1, devices, greet, 0)
    return barrier


def wait_bytes(ref, sem):
    pltpu.make_async_copy(ref, ref, sem).wait()


def send_block(src, dst, send_sem, recv_sem, peer, narrow_count):
    pltpu.make_async_remote_copy(
        src_ref=src,
        dst_ref=dst,
        send_sem=send_sem,
        recv_sem=recv_sem,
        device_id=place(peer, narrow_count),
        device_id_type=MESH,
    ).start()


def scatter_kernel(unroll, parts, order_ref, dups_ref, rows_any, out_ref, dup_ref,
                   rows_in, wide_in, wide_out, sems):
    count = rows_in.shape[0]
    part = count // parts
    copies = [
        pltpu.make_async_copy(
            rows_any.at[pl.ds(p * part, part)], rows_in.at[pl.ds(p * part, part)], sems.at[p]
        )
        for p in range(parts)
    ]
    for copy in copies:
        copy.start()
    dup_ref[0] = dups_ref[0, 0]

    def move(step, carry):
        base = pl.multiple_of(step * unroll, unroll)
        for u in range(unroll):
            target = order_ref[base + u]
            wide_out[pl.ds(target, 1), :] = wide_in[pl.ds(base + u, 1), :]
        return carry

    for p, copy in enumerate(copies):
        copy.wait()
        at = pl.ds(p * part, part)
        wide_in[at, :] = rows_in[at, :].astype(jnp.float32)
        lax.fori_loop(p * part // unroll, (p + 1) * part // unroll, move, 0)
    out_ref[...] = wide_out[...].astype(out_ref.dtype)


def scatter_rows(order, dups, rows):
    count, cols = rows.shape
    parts = 4
    return pl.pallas_call(
        functools.partial(scatter_kernel, 16, parts),
        out_shape=(
            jax.ShapeDtypeStruct(rows.shape, rows.dtype),
            jax.ShapeDtypeStruct((1,), jnp.int32),
        ),
        in_specs=[
            pl.BlockSpec(memory_space=SMEM),
            pl.BlockSpec(memory_space=VMEM),
            pl.BlockSpec(memory_space=pl.ANY),
        ],
        out_specs=(pl.BlockSpec(memory_space=VMEM), pl.BlockSpec(memory_space=SMEM)),
        scratch_shapes=[
            VMEM((count, cols), rows.dtype),
            VMEM((count, cols), jnp.float32),
            VMEM((count, cols), jnp.float32),
            pltpu.SemaphoreType.DMA((parts,)),
        ],
        compiler_params=pltpu.CompilerParams(vmem_limit_bytes=16 * 1024 * 1024),
    )(order, dups, rows)


def exchange_kernel(
    devices, narrow_count, chunks, groups, tile,
    order_ref, payload_any, sent_one, sent_two,
    back_ref, dup_ref,
    rows_ref, wide_in, wide_slot, got_one, got_two,
    got, totals, means, col_one, col_two, lane_one, lane_two, wide_rows, dup_mine, dup_all,
    payload_ref, load_sem, tag_send, tag_recv,
    send_sem, recv_sems, back_send, back_recv, dup_send, dup_recv,
):
    _, slot_rows, cols = rows_ref.shape
    count = devices * slot_rows
    chunk_slots = devices // chunks
    lanes = lane_one.shape[1]
    me = my_flat(narrow_count)
    my_chunk = me // chunk_slots
    unit_slots = max(1, lanes // slot_rows)
    unit_rows = unit_slots * slot_rows
    units = chunk_slots // unit_slots
    group_units = units // groups
    group_slots = devices // groups
    my_unit = me % chunk_slots // unit_slots
    load = pltpu.make_async_copy(payload_any, payload_ref, load_sem)
    load.start()
    barrier = greet_all(me, devices, narrow_count)
    load.wait()
    wide_in[...] = payload_ref[...].astype(jnp.float32)
    pl.semaphore_wait(barrier, devices - 1)

    pltpu.make_async_copy(sent_one.at[me], got_one.at[me], tag_recv.at[0]).start()
    pltpu.make_async_copy(sent_two.at[me], got_two.at[me], tag_recv.at[1]).start()

    def send_tags(step, carry):
        peer = (me + step) % devices
        send_block(
            sent_one.at[peer], got_one.at[me], tag_send.at[0], tag_recv.at[0], peer, narrow_count
        )
        send_block(
            sent_two.at[peer], got_two.at[me], tag_send.at[1], tag_recv.at[1], peer, narrow_count
        )
        return carry

    lax.fori_loop(1, devices, send_tags, 0)

    def peer_of(step):
        rest = step % group_slots
        turn = rest // chunks
        first = (my_chunk + rest % chunks) % chunks * chunk_slots
        offset = step // group_slots * group_units + turn // unit_slots
        unit = (my_unit + offset) % units
        return step // group_slots, first + unit * unit_slots + (me + turn) % unit_slots

    def send_slot(step):
        group, peer = peer_of(step)
        send_block(
            rows_ref.at[peer], got.at[me], send_sem, recv_sems.at[group], peer, narrow_count
        )

    unroll = min(16, slot_rows)

    def fill(step, carry):
        _, peer = peer_of(step)

        def move(inner, carry):
            base = pl.multiple_of(inner * unroll, unroll)
            for u in range(unroll):
                source = order_ref[peer * slot_rows + base + u]
                wide_slot[pl.ds(base + u, 1), :] = wide_in[pl.ds(source, 1), :]
            return carry

        lax.fori_loop(0, slot_rows // unroll, move, 0)
        rows_ref[peer] = wide_slot[...].astype(rows_ref.dtype)

        @pl.when(step > 1)
        def _():
            send_slot(step - 1)

        return carry

    lax.fori_loop(0, devices, fill, 0)
    pltpu.make_async_copy(rows_ref.at[me], got.at[me], recv_sems.at[0]).start()

    wait_bytes(got_one, tag_recv.at[0])
    send_slot(devices - 1)
    wait_bytes(got_two, tag_recv.at[1])
    if slot_rows >= lanes:
        per_slot = slot_rows // lanes
        for r in range(count // lanes):
            piece = pl.ds(r % per_slot * lanes, lanes)
            lane_one[r : r + 1, :] = got_one[r // per_slot, :, piece]
            lane_two[r : r + 1, :] = got_two[r // per_slot, :, piece]
    else:
        group = lanes // slot_rows
        for r in range(count // lanes):
            pieces = range(r * group, (r + 1) * group)
            lane_one[r : r + 1, :] = jnp.concatenate([got_one[p] for p in pieces], axis=1)
            lane_two[r : r + 1, :] = jnp.concatenate([got_two[p] for p in pieces], axis=1)
    one = lane_one[...]
    flipped_one = one.T
    flipped_two = lane_two[...].T
    lane_one[...] = jnp.where(one < 0, -2, one)
    for r in range(count // lanes):
        at = pl.ds(r * lanes, lanes)
        col_one[at, :] = jnp.broadcast_to(flipped_one[:, r : r + 1], (lanes, lanes))
        col_two[at, :] = jnp.broadcast_to(flipped_two[:, r : r + 1], (lanes, lanes))
    wide_rows[:, cols:] = jnp.ones((group_slots * slot_rows, cols), wide_rows.dtype)
    dup_mine[...] = jnp.zeros_like(dup_mine)

    tiles = count // tile
    tile_slots = tile // slot_rows

    def send_tile(index):
        for u in range(tile_slots):
            peer = index * tile_slots + u

            @pl.when(peer == me)
            def _():
                pltpu.make_async_copy(means.at[peer], back_ref.at[me], back_recv).start()

            @pl.when(peer != me)
            def _():
                send_block(
                    means.at[peer], back_ref.at[me], back_send, back_recv, peer, narrow_count
                )

    plane_tiles = tiles // chunks

    def tile_of(step):
        plane = (my_chunk + step) % chunks
        return plane * plane_tiles + (me + step // chunks) % plane_tiles

    for g in range(groups):
        wait_bytes(got.at[pl.ds(0, group_slots)], recv_sems.at[g])
        lane_bases = []
        for c in range(chunks):
            for o in range(group_units):
                unit = (my_unit - g * group_units - o + 2 * units) % units
                first = (my_chunk + c) % chunks * chunk_slots + unit * unit_slots
                to = pl.ds(len(lane_bases) * unit_rows, unit_rows)
                wide_rows[to, :cols] = got[pl.ds(first, unit_slots)].reshape(unit_rows, cols)
                lane_bases.append(first * slot_rows // lanes)

        def body(step, carry, g=g, lane_bases=tuple(lane_bases)):
            index = tile_of(step)
            at = pl.ds(pl.multiple_of(index * tile, tile), tile)
            left_one = col_one[at, :]
            left_two = col_two[at, :]
            parts = []
            for b in range(group_slots * slot_rows // lanes):
                per_unit = unit_rows // lanes
                row_at = pl.ds(lane_bases[b // per_unit] + b % per_unit, 1)
                same = (left_one == lane_one[row_at, :]) & (left_two == lane_two[row_at, :])
                parts.append(jnp.where(same, 1.0, 0.0).astype(jnp.bfloat16))
            mask = jnp.concatenate(parts, axis=1)
            part = jnp.dot(mask, wide_rows[...], preferred_element_type=jnp.float32)
            if g > 0:
                part = part + totals[at, :]
            if g < groups - 1:
                totals[at, :] = part
            else:
                sums = part[:, :cols]
                counts = part[:, cols:]
                floor = jnp.maximum(counts, 1.0)
                mean = (sums / floor).astype(means.dtype)
                means[pl.ds(index * tile_slots, tile_slots)] = mean.reshape(
                    tile_slots, slot_rows, cols
                )
                held = jnp.where(counts > 0.0, 1.0, 0.0)
                dup_mine[0] += jnp.sum(held.reshape(tile // 8, 8, cols), axis=0)
                dup_mine[1] += jnp.sum((held / floor).reshape(tile // 8, 8, cols), axis=0)

                @pl.when(step > 0)
                def _():
                    send_tile(tile_of(step - 1))
            return carry

        lax.fori_loop(0, tiles, body, 0)

    live_rows = jnp.sum(dup_mine[0], axis=0, keepdims=True)
    groups = jnp.floor(jnp.sum(dup_mine[1], axis=0, keepdims=True) + 0.5)
    dup_mine[0] = jnp.broadcast_to(live_rows - groups, (8, cols))
    send_tile(tile_of(tiles - 1))
    pltpu.make_async_copy(dup_mine.at[0], dup_all.at[me], dup_recv).start()

    def send_dup(step, carry):
        peer = (me + step) % devices
        send_block(dup_mine.at[0], dup_all.at[me], dup_send, dup_recv, peer, narrow_count)
        return carry

    lax.fori_loop(1, devices, send_dup, 0)
    wait_bytes(dup_all, dup_recv)
    dup_ref[...] = jnp.sum(dup_all[...], axis=0).astype(jnp.int32)
    wait_bytes(back_ref, back_recv)
    wait_bytes(sent_one.at[pl.ds(0, devices - 1)], tag_send.at[0])
    wait_bytes(sent_two.at[pl.ds(0, devices - 1)], tag_send.at[1])
    wait_bytes(rows_ref.at[pl.ds(0, devices - 1)], send_sem)
    wait_bytes(means.at[pl.ds(0, devices - 1)], back_send)
    wait_bytes(dup_all.at[pl.ds(0, devices - 1)], dup_send)


def on_device(payload, first_key, second_key, live, first_bucket, second_bucket):
    wide_count = lax.axis_size("wide")
    narrow_count = lax.axis_size("narrow")
    devices = wide_count * narrow_count
    row_count, cols = payload.shape
    slot_rows = row_count // devices
    owner = first_bucket * narrow_count + second_bucket
    packed = owner * row_count + lax.iota(jnp.int32, row_count)
    packed, key_one, key_two = lax.sort(
        (packed, jnp.where(live > 0, first_key, -1), second_key), num_keys=1, is_stable=False
    )
    order = packed % row_count
    lanes = 128
    tags = (devices, 1, slot_rows)
    unit_slots = max(1, lanes // slot_rows)
    chunks = 4 if devices % (4 * unit_slots) == 0 else 1
    groups = 4 if devices % (4 * chunks * unit_slots) == 0 else 1
    tile = max(256, slot_rows)
    tile = min(tile, row_count)
    block = (devices, slot_rows, cols)
    back, dups = pl.pallas_call(
        functools.partial(exchange_kernel, devices, narrow_count, chunks, groups, tile),
        out_shape=(
            jax.ShapeDtypeStruct(block, payload.dtype),
            jax.ShapeDtypeStruct((8, cols), jnp.int32),
        ),
        in_specs=[
            pl.BlockSpec(memory_space=SMEM),
            pl.BlockSpec(memory_space=pltpu.HBM),
            pl.BlockSpec(memory_space=VMEM),
            pl.BlockSpec(memory_space=VMEM),
        ],
        out_specs=(pl.BlockSpec(memory_space=VMEM), pl.BlockSpec(memory_space=VMEM)),
        scratch_shapes=[
            VMEM(block, payload.dtype),
            VMEM((row_count, cols), jnp.float32),
            VMEM((slot_rows, cols), jnp.float32),
            VMEM(tags, jnp.int32),
            VMEM(tags, jnp.int32),
            VMEM(block, payload.dtype),
            VMEM((row_count, 2 * cols), jnp.float32),
            VMEM(block, payload.dtype),
            VMEM((row_count, lanes), jnp.int32),
            VMEM((row_count, lanes), jnp.int32),
            VMEM((row_count // lanes, lanes), jnp.int32),
            VMEM((row_count // lanes, lanes), jnp.int32),
            VMEM((row_count // groups, 2 * cols), payload.dtype),
            VMEM((2, 8, cols), jnp.float32),
            VMEM((devices, 8, cols), jnp.float32),
            VMEM((row_count, cols), payload.dtype),
            pltpu.SemaphoreType.DMA,
            pltpu.SemaphoreType.DMA((2,)),
            pltpu.SemaphoreType.DMA((2,)),
            pltpu.SemaphoreType.DMA,
            pltpu.SemaphoreType.DMA((groups,)),
            pltpu.SemaphoreType.DMA,
            pltpu.SemaphoreType.DMA,
            pltpu.SemaphoreType.DMA,
            pltpu.SemaphoreType.DMA,
        ],
        compiler_params=pltpu.CompilerParams(
            collective_id=0, has_side_effects=True, vmem_limit_bytes=48 * 1024 * 1024
        ),
    )(order, payload, key_one.reshape(tags), key_two.reshape(tags))
    group_mean, total = scatter_rows(order, dups, back.reshape(row_count, cols))
    return (group_mean, total[0])


def solution(mesh):
    placed = (
        P(("wide", "narrow"), None),
        P(("wide", "narrow")),
        P(("wide", "narrow")),
        P(("wide", "narrow")),
        P(("wide", "narrow")),
        P(("wide", "narrow")),
    )
    return jax.shard_map(
        on_device,
        mesh=mesh,
        in_specs=placed,
        out_specs=(P(("wide", "narrow"), None), P()),
        check_vma=False,
    )
```
